32 devices in a mesh: fft: 8 (over z, y), band: 4 (over x, core).
Axes of the slice: x: 2, y: 2, z: 4, core: 2. Of those that a mesh axis runs over, the one named last changes fastest.
Arguments:
- coefficients: bfloat16 [48, 184320], P('band', 'fft'), may hold values from -0.078125 to 0.078125
- occupations: float32 [48], P('band'), may hold values from 0.5 to 2
- columns: int32 [1280], P('fft'), may hold values from 0 to 5183
- counts: int32 [8], P('fft'), may hold values from 1 to 160, 512 in all
- plane_slot: int32 [144], replicated, may hold values from -1 to 143, as said below
Outputs:
- density: float32 [144, 144, 144], P('fft', 'band')
The draws below stay inside these ranges and needn't reach their ends.
Inputs may be any that keep to these rules, and one draw needn't show every extreme that they name: The counts sum to 512, and one of them equals 160. `plane_slot`: every plane 0 .. 143 stands in exactly one slot; the other slots hold -1.
All inputs are finite; a program needn't handle non-finite values. No bound on the sum of `counts` on one device may be relied on, other than what follows from the above.
Results may differ from the reference program's by a relative error of at most 0.0095.
Values may be sent and summed in bfloat16 or wider, within the bound.
A program may use at most 192 MiB of HBM per device.

```python
import math
import jax
import jax.numpy as jnp
import numpy as np
from jax import lax

N = 144
GB = 72
STICK_DEV = 160
STICKS = 512
STICKS_ALL = 1280
BANDS = 48
SLOTS = 144
N_FFT = 8


def draw_plane_slot(key, part):
    shuffled = jax.random.permutation(key, SLOTS)
    return jnp.where(shuffled < N, shuffled, -1).astype(jnp.int32)


def touch_ends(values, stream_key, least, high):
    longest = values.shape.index(max(values.shape))
    spots = []
    for shift in (0, 1):
        where = [jax.random.randint(jax.random.fold_in(stream_key, axis), (), 0, length) for axis, length in enumerate(values.shape)]
        where[longest] = (where[longest] + shift) % values.shape[longest]
        spots.append(tuple(where))
    return values.at[spots[0]].set(least).at[spots[1]].set(high)


def block_levels(rng, dims, cuts, least, top_value):
    def one(dim, parts):
        draws = jax.random.uniform(jax.random.fold_in(jax.random.fold_in(rng, 6), dim), (parts,), jnp.float32, least / len(cuts), top_value / len(cuts))
        return jnp.repeat(jnp.exp(draws), dims[dim] // parts).reshape((-1,) + (1,) * (len(dims) - dim - 1))

    loudness = one(*cuts[0])
    for cut in cuts[1:]:
        loudness = loudness * one(*cut)
    return loudness


def length_profile(count, total, limit, slope):
    loads = [(1 << 20) // math.isqrt(rank ** slope) + 1 for rank in range(2, count + 1)]
    surplus, given = total - limit - (count - 1), [1] * (count - 1)
    while surplus > 0:
        free = [i for i in range(count - 1) if given[i] < limit]
        mass, budget = sum([loads[i] for i in free]), surplus
        for i in free:
            extra = min(limit - given[i], max(1, budget * loads[i] // mass), surplus)
            given[i] = given[i] + extra
            surplus = surplus - extra
    return np.array([limit] + given)


def ragged_sizes(rng, count, total, reach, slope):
    if count == 2:
        one = jax.random.randint(rng, (), max(1, total - reach), min(reach, total - 1) + 1)
        return jnp.stack([one, total - one])
    lengths = jnp.asarray(length_profile(count, total, reach, slope), jnp.int32)
    twos = (count - 1) // 2
    donor, receiver = lengths[1:1 + 2 * twos:2], lengths[2:2 + 2 * twos:2]
    room = jnp.minimum(donor - 1, reach - receiver)
    shifted = jax.random.randint(jax.random.fold_in(rng, 1), (twos,), 0, 1 << 20) % (room + 1)
    lengths = lengths.at[1:1 + 2 * twos:2].set(donor - shifted).at[2:2 + 2 * twos:2].set(receiver + shifted)
    return lengths[jax.random.permutation(jax.random.fold_in(rng, 2), count)]


def scatter_about(stream_key, shape, width, limit, shards=(), kind=jnp.bfloat16):
    level = block_levels(stream_key, shape, shards, -0.22, 0.18) if shards else 1.0
    entries = jax.random.normal(stream_key, shape, jnp.float32) * width * level
    return jnp.minimum(jnp.maximum(entries, -limit), limit).astype(kind)


def setup_inputs(seed: int = 0) -> dict:
    streams_of = jax.random.split(jax.random.key(seed), 6)
    coefficients = scatter_about(streams_of[0], (BANDS, STICKS_ALL * 2 * GB), (1.0 / (STICKS * GB) ** 0.5), 0.078125, ((0, 4), (1, 8)))
    occupations = jnp.clip(jnp.exp(math.log(2.0) - 1.3862944 * jax.random.uniform(streams_of[1], (BANDS,), jnp.float32) ** block_levels(streams_of[1], (BANDS,), ((0, 4),), -0.2, 0.2)), 0.5, 2.0)
    columns = touch_ends(jax.random.randint(streams_of[2], (STICKS_ALL,), 0, GB * GB), jax.random.fold_in(streams_of[2], 1), 0, (GB * GB) - 1).astype(jnp.int32)
    counts = ragged_sizes(streams_of[3], N_FFT, STICKS, STICK_DEV, 2).astype(jnp.int32)
    plane_slot = draw_plane_slot(jax.random.fold_in(streams_of[5], 71), 0)
    return {"coefficients": coefficients, "occupations": occupations, "columns": columns, "counts": counts, "plane_slot": plane_slot}


def phase_pair(freq_count, positions, grid):
    freqs = jnp.arange(freq_count, dtype=jnp.int32) - freq_count // 2
    turns = jnp.mod(freqs[:, None] * positions[None, :], grid)
    angles = turns.astype(jnp.float32) * (2.0 * math.pi / grid)
    return jnp.cos(angles), jnp.sin(angles)


def stick_table(plane_slot):
    valid_slot = (plane_slot >= 0).astype(jnp.float32)
    cosine, sine_part = phase_pair(GB, jnp.maximum(plane_slot, 0), N)
    cosine = cosine * valid_slot[None, :]
    sine_part = sine_part * valid_slot[None, :]
    upper_rows = jnp.concatenate([cosine, sine_part], axis=1)
    lower_rows = jnp.concatenate([-sine_part, cosine], axis=1)
    return jnp.concatenate([upper_rows, lower_rows], axis=0).astype(jnp.bfloat16)


def row_table():
    cosine, sine_part = phase_pair(GB, jnp.arange(N, dtype=jnp.int32), N)
    upper_rows = jnp.concatenate([cosine, sine_part], axis=1)
    lower_rows = jnp.concatenate([-sine_part, cosine], axis=1)
    return jnp.concatenate([upper_rows, lower_rows], axis=0).astype(jnp.bfloat16)


def column_table():
    cosine, sine_part = phase_pair(GB, jnp.arange(N, dtype=jnp.int32), N)
    return jnp.concatenate([cosine.T, sine_part.T], axis=0).astype(jnp.bfloat16)


def grid_squares(received, real_index, imag_index, row_tab, col_tab):
    bands_here, _, planes, _ = received.shape
    flat_plane = jnp.zeros((bands_here, planes, GB * 2 * GB), jnp.float32)
    flat_plane = flat_plane.at[:, :, real_index].add(received[:, 0].astype(jnp.float32))
    flat_plane = flat_plane.at[:, :, imag_index].add(received[:, 1].astype(jnp.float32))
    g_plane = flat_plane.reshape(bands_here, planes, GB, 2 * GB).astype(jnp.bfloat16)
    half_way = jnp.einsum("bpgk,kj->bpgj", g_plane.astype(jnp.float32), row_tab.astype(jnp.float32)).astype(jnp.bfloat16)
    full_grid = jnp.einsum("xg,bpgj->bpxj", col_tab.astype(jnp.float32), half_way.astype(jnp.float32))
    real_part = full_grid[:, :, :N, :N] - full_grid[:, :, N:, N:]
    imag_part = full_grid[:, :, N:, :N] + full_grid[:, :, :N, N:]
    return real_part * real_part + imag_part * imag_part


def reference(coefficients, occupations, columns, counts, plane_slot):
    shaped = coefficients.reshape(BANDS, STICKS_ALL, 2 * GB)
    stick_place = jnp.arange(STICKS_ALL, dtype=jnp.int32)
    live_stick = (stick_place % STICK_DEV < jnp.repeat(counts, STICK_DEV)).astype(jnp.bfloat16)
    masked = shaped * live_stick[None, :, None]
    real_index = (columns // GB) * (2 * GB) + columns % GB
    imag_index = real_index + GB
    plane_tab = stick_table(plane_slot)
    row_tab = row_table()
    col_tab = column_table()

    def one_band(running, inputs):
        coeffs, weight = inputs
        sticks = jnp.dot(coeffs, plane_tab, preferred_element_type=jnp.float32).astype(jnp.bfloat16)
        outgoing = sticks.T.reshape(1, 2, SLOTS, STICKS_ALL)
        squares = grid_squares(outgoing, real_index, imag_index, row_tab, col_tab)
        return running + weight * squares[0], None

    start = jnp.zeros((SLOTS, N, N), jnp.float32)
    density, _ = lax.scan(one_band, start, (masked, occupations / BANDS))
    return density
```

```python
import functools
import math

import jax
import jax.numpy as jnp
from jax import lax
from jax.experimental import pallas as pl
from jax.experimental.pallas import tpu as pltpu
from jax.sharding import PartitionSpec as P

N = 144
GB = 72
LIVE_PER_DEVICE = 64
GP = 80
YP = 256
META = 8


def phase_pair(freq_count, positions, grid):
    freqs = jnp.arange(freq_count, dtype=jnp.int32) - freq_count // 2
    turns = jnp.mod(freqs[:, None] * positions[None, :], grid)
    angles = turns.astype(jnp.float32) * (2.0 * math.pi / grid)
    return (jnp.cos(angles), jnp.sin(angles))


def stick_table(plane_slot, groups):
    valid_slot = (plane_slot >= 0).astype(jnp.float32)
    cosine, sine_part = phase_pair(GB, jnp.maximum(plane_slot, 0), N)
    cosine = cosine * valid_slot[None, :]
    sine_part = sine_part * valid_slot[None, :]
    upper = jnp.stack([cosine, sine_part], axis=-1)
    lower = jnp.stack([-sine_part, cosine], axis=-1)
    return jnp.concatenate([upper, lower], axis=0).astype(jnp.bfloat16)


def row_table():
    cosine, sine_part = phase_pair(GB, jnp.arange(N, dtype=jnp.int32), N)
    pad = lambda a: jnp.pad(a, ((0, GP - GB), (0, YP - N)))
    return jnp.concatenate(
        [pad(cosine), pad(sine_part), pad(-sine_part), pad(cosine)], axis=1
    ).astype(jnp.bfloat16)


def column_table():
    cosine, sine_part = phase_pair(GB, jnp.arange(N, dtype=jnp.int32), N)
    pad = lambda a: jnp.pad(a.T, ((0, 0), (0, GP - GB)))
    upper = jnp.concatenate([pad(cosine), pad(-sine_part)], axis=1)
    lower = jnp.concatenate([pad(sine_part), pad(cosine)], axis=1)
    return jnp.concatenate([upper, lower], axis=0).astype(jnp.bfloat16)


def grid_kernel(bands, live, weights, recv, row_tab, col_tab, out, sticks, table, masked, row_hot):
    plane = pl.program_id(0)
    sources, rows, here = recv.shape
    data_rows = rows - META

    @pl.when(plane == 0)
    def _():
        total = jnp.zeros((rows, live), jnp.float32)
        offset = jnp.zeros((1, 1), jnp.float32)
        target = lax.broadcasted_iota(jnp.int32, (live, here), 0).astype(jnp.float32)
        place = lax.broadcasted_iota(jnp.int32, (live, here), 1).astype(jnp.float32)
        for source in range(sources):
            block = recv[source]
            alive = block[data_rows:, :].astype(jnp.float32)[2:3, :]
            pick = jnp.where(target == place + offset, 1.0, 0.0) * alive
            total += lax.dot_general(
                block,
                pick.astype(jnp.bfloat16),
                (((1,), (1,)), ((), ())),
                preferred_element_type=jnp.float32,
            )
            offset += jnp.sum(alive, axis=1, keepdims=True)
        sticks[...] = total[:data_rows].reshape(sticks.shape)
        meta = total[data_rows:]
        freq = lax.broadcasted_iota(jnp.int32, (GP, live), 0).astype(jnp.float32)
        row_hot[...] = jnp.where(freq == meta[0:1, :], 1.0, 0.0)
        col_hot = jnp.where(freq == meta[1:2, :], 1.0, 0.0).astype(jnp.bfloat16)
        for part in range(2):
            table[part * live : (part + 1) * live, :] = lax.dot_general(
                col_hot,
                row_tab[:, 2 * YP * part : 2 * YP * (part + 1)],
                (((0,), (0,)), ((), ())),
                preferred_element_type=jnp.float32,
            ).astype(jnp.bfloat16)

    mine = sticks[plane]
    hot = row_hot[...]
    for part in range(2):
        for band in range(bands):
            row = mine[part * bands + band : part * bands + band + 1, :]
            masked[band * GP : (band + 1) * GP, part * live : (part + 1) * live] = (
                hot * row
            ).astype(jnp.bfloat16)
    half = jnp.dot(masked[...], table[...], preferred_element_type=jnp.float32)
    half = half.astype(jnp.bfloat16)
    density = jnp.zeros((N, YP), jnp.float32)
    for band in range(bands):
        piece = half[band * GP : (band + 1) * GP, :]
        stacked = jnp.concatenate([piece[:, :YP], piece[:, YP:]], axis=0)
        wave = jnp.dot(col_tab[...], stacked, preferred_element_type=jnp.float32)
        real, imag = wave[:N], wave[N:]
        density += weights[band] * (real * real + imag * imag)
    owners, _, own_rows, _ = out.shape
    for owner in range(owners):
        out[owner, 0] = density[owner * own_rows : (owner + 1) * own_rows, :N].astype(out.dtype)


def shards(coefficients, occupations, columns, counts, plane_slot):
    bands = coefficients.shape[0]
    here = columns.shape[0]
    ways = lax.axis_size("fft")
    groups = lax.axis_size("band")
    planes = plane_slot.shape[0] // ways
    live = LIVE_PER_DEVICE * ways
    coefficients = coefficients.reshape(bands, here, 2 * GB)
    plane_tab = stick_table(plane_slot, ways)
    weights = occupations / (bands * groups)
    made = jnp.einsum(
        "gjc,bsg->jcbs", plane_tab, coefficients, preferred_element_type=jnp.float32
    ).astype(jnp.bfloat16)
    made = made.reshape(ways, planes * 2 * bands, here)
    alive = jnp.arange(here, dtype=jnp.int32) < counts[0]
    meta = jnp.stack([columns // GB, columns % GB, alive.astype(jnp.int32)]).astype(jnp.bfloat16)
    meta = jnp.pad(meta, ((0, META - 3), (0, 0)))
    outgoing = jnp.concatenate(
        [made, jnp.broadcast_to(meta[None], (ways, META, here))], axis=1
    )
    received = lax.all_to_all(outgoing, "fft", split_axis=0, concat_axis=0, tiled=True)
    rows = N // groups
    whole = pl.BlockSpec(memory_space=pltpu.VMEM)
    local = pl.pallas_call(
        functools.partial(grid_kernel, bands, live),
        grid=(planes,),
        in_specs=[pl.BlockSpec(memory_space=pltpu.SMEM), whole, whole, whole],
        out_specs=pl.BlockSpec((groups, 1, rows, N), lambda p: (0, p, 0, 0)),
        out_shape=jax.ShapeDtypeStruct((groups, planes, rows, N), jnp.bfloat16),
        scratch_shapes=[
            pltpu.VMEM((planes, 2 * bands, live), jnp.float32),
            pltpu.VMEM((2 * live, 2 * YP), jnp.bfloat16),
            pltpu.VMEM((bands * GP, 2 * live), jnp.bfloat16),
            pltpu.VMEM((GP, live), jnp.float32),
        ],
        compiler_params=pltpu.CompilerParams(vmem_limit_bytes=60 * 1024 * 1024),
        name="grid",
    )(weights, received, row_table(), column_table())
    swapped = lax.all_to_all(local, "band", split_axis=0, concat_axis=0, tiled=True)
    return jnp.sum(swapped.astype(jnp.float32), axis=0)


def solution(mesh):
    placed = (P("band", "fft"), P("band"), P("fft"), P("fft"), P())
    return jax.shard_map(
        shards, mesh=mesh, in_specs=placed, out_specs=P("fft", "band", None), check_vma=False
    )
```

```python
import functools
import math

import jax
import jax.numpy as jnp
import numpy as np
from jax import lax
from jax.experimental import pallas as pl
from jax.experimental.pallas import tpu as pltpu
from jax.sharding import PartitionSpec as P

N = 144
GB = 72
HALF = N // 2
LIVE_PER_DEVICE = 64
GP = 80
LANES = 128
META = 16
MESH = pl.DeviceIdType.MESH


def phase_pair(freq_count, positions, grid):
    freqs = jnp.arange(freq_count, dtype=jnp.int32) - freq_count // 2
    turns = jnp.mod(freqs[:, None] * positions[None, :], grid)
    angles = turns.astype(jnp.float32) * (2.0 * math.pi / grid)
    return (jnp.cos(angles), jnp.sin(angles))


def stick_table(plane_slot):
    valid_slot = (plane_slot >= 0).astype(jnp.float32)
    cosine, sine_part = phase_pair(GB, jnp.maximum(plane_slot, 0), N)
    cosine = cosine * valid_slot[None, :]
    sine_part = sine_part * valid_slot[None, :]
    upper = jnp.stack([cosine, sine_part], axis=-1)
    lower = jnp.stack([-sine_part, cosine], axis=-1)
    return jnp.concatenate([upper, lower], axis=0).astype(jnp.bfloat16)


def fixed_phases():
    freqs = np.arange(GB, dtype=np.int64) - GB // 2
    turns = np.mod(freqs[:, None] * np.arange(N)[None, :], N)
    angles = turns * (2.0 * math.pi / N)
    return np.cos(angles), np.sin(angles)


def row_table():
    cosine, sine_part = fixed_phases()
    table = np.zeros((GP, 2 * LANES))
    table[:GB, : HALF + 1] = cosine[:, : HALF + 1]
    table[:GB, LANES : LANES + HALF + 1] = sine_part[:, : HALF + 1]
    return jnp.asarray(table.astype(jnp.bfloat16))


def column_table():
    cosine, sine_part = fixed_phases()
    table = np.zeros((2 * N, 2 * GP))
    table[:N, :GB] = cosine.T
    table[:N, GP : GP + GB] = -sine_part.T
    table[N:, :GB] = sine_part.T
    table[N:, GP : GP + GB] = cosine.T
    return jnp.asarray(table.astype(jnp.bfloat16))


def order_table():
    table = np.zeros((2 * LANES, N))
    for y in range(N):
        table[y if y <= HALF else LANES + N - y, y] = 1.0
    return jnp.asarray(table.astype(jnp.bfloat16))


def grid_kernel(
    bands, live, chunk_planes, ways, groups,
    weights, outgoing, meta_out, row_tab, col_tab, order,
    out,
    recv, meta_in, sticks, table, masked, row_hot, sent, landed,
    meta_send, meta_recv, go_send, go_recv, sum_send, sum_recv,
):
    plane = pl.program_id(0)
    planes = pl.num_programs(0)
    total_planes = out.shape[0]
    chunks = total_planes // chunk_planes
    chunk_rows = chunk_planes * 2 * bands
    here = recv.shape[-1]
    me = lax.axis_index("fft")
    group = lax.axis_index("band")

    def meta_copy(step, source):
        peer = lax.rem(me + step, ways)
        return pltpu.make_async_remote_copy(
            src_ref=meta_out, dst_ref=meta_in.at[source],
            send_sem=meta_send.at[step - 1], recv_sem=meta_recv.at[source],
            device_id={"fft": peer}, device_id_type=MESH,
        )

    def stick_copy(chunk, step, source):
        peer = lax.rem(me + step, ways)
        return pltpu.make_async_remote_copy(
            src_ref=outgoing.at[peer, pl.ds(chunk * chunk_rows, chunk_rows)],
            dst_ref=recv.at[chunk, source],
            send_sem=go_send.at[chunk, step - 1], recv_sem=go_recv.at[chunk, source],
            device_id={"fft": peer}, device_id_type=MESH,
        )

    def sum_copy(which, step, source):
        peer = lax.rem(group + step, groups)
        return pltpu.make_async_remote_copy(
            src_ref=sent.at[peer, which], dst_ref=landed.at[source, which],
            send_sem=sum_send.at[which, step - 1], recv_sem=sum_recv.at[which, source],
            device_id={"band": peer}, device_id_type=MESH,
        )

    @pl.when(plane == 0)
    def _():
        barrier = pltpu.get_barrier_semaphore()
        for step in range(1, ways):
            pl.semaphore_signal(
                barrier, inc=1, device_id={"fft": lax.rem(me + step, ways)}, device_id_type=MESH
            )
        for step in range(1, groups):
            pl.semaphore_signal(
                barrier, inc=1, device_id={"band": lax.rem(group + step, groups)},
                device_id_type=MESH,
            )
        pl.semaphore_wait(barrier, ways + groups - 2)
        for step in range(1, ways):
            meta_copy(step, me).start()
        for chunk in range(chunks):
            for step in range(1, ways):
                stick_copy(chunk, step, me).start()
        meta_in[me] = meta_out[...]
        for chunk in range(chunks):
            recv[chunk, me] = outgoing[me, chunk * chunk_rows : (chunk + 1) * chunk_rows]
        for step in range(1, ways):
            meta_copy(step, lax.rem(me + ways - step, ways)).wait()

    @pl.when(lax.rem(plane, chunk_planes) == 0)
    def _():
        chunk = plane // chunk_planes
        for step in range(1, ways):
            stick_copy(chunk, step, lax.rem(me + ways - step, ways)).wait()
        offset = jnp.zeros((1, 1), jnp.float32)
        target = lax.broadcasted_iota(jnp.int32, (live, here), 0).astype(jnp.float32)
        place = lax.broadcasted_iota(jnp.int32, (1, here), 1).astype(jnp.float32)
        total = jnp.zeros((chunk_rows, live), jnp.float32)
        facts = jnp.zeros((META, live), jnp.float32)
        for source in range(ways):
            meta = meta_in[source]
            alive = meta.astype(jnp.float32)[2:3, :]
            spot = jnp.where(alive > 0.5, place + offset, -1.0)
            pick = jnp.where(target == spot, 1.0, 0.0).astype(jnp.bfloat16)
            turn = (((1,), (1,)), ((), ()))
            total += lax.dot_general(
                recv[chunk, source], pick, turn, preferred_element_type=jnp.float32
            )
            facts += lax.dot_general(meta, pick, turn, preferred_element_type=jnp.float32)
            offset += jnp.sum(alive, axis=1, keepdims=True)
        sticks[...] = total.reshape(sticks.shape)

        @pl.when(plane == 0)
        def _():
            freq = lax.broadcasted_iota(jnp.int32, (GP, live), 0).astype(jnp.float32)
            row_hot[...] = jnp.where(freq == facts[0:1, :], 1.0, 0.0)
            col_hot = jnp.where(freq == facts[1:2, :], 1.0, 0.0).astype(jnp.bfloat16)
            table[...] = lax.dot_general(
                col_hot, row_tab[...], (((0,), (0,)), ((), ())),
                preferred_element_type=jnp.float32,
            ).astype(jnp.bfloat16)

    mine = sticks[lax.rem(plane, chunk_planes)]
    hot = row_hot[...]
    for index in range(2 * bands):
        masked[index * GP : (index + 1) * GP, :] = (hot * mine[index : index + 1, :]).astype(
            jnp.bfloat16
        )
    made = jnp.dot(masked[...], table[...], preferred_element_type=jnp.float32)
    density = jnp.zeros((N, 2 * LANES), jnp.float32)
    for band in range(bands):
        real_in = made[band * GP : (band + 1) * GP]
        imag_in = made[(bands + band) * GP : (bands + band + 1) * GP]
        rc, rs = real_in[:, :LANES], real_in[:, LANES:]
        ic, im = imag_in[:, :LANES], imag_in[:, LANES:]
        stacked = jnp.concatenate(
            [
                jnp.concatenate([rc - im, rc + im], axis=1),
                jnp.concatenate([ic + rs, ic - rs], axis=1),
            ],
            axis=0,
        ).astype(jnp.bfloat16)
        wave = jnp.dot(col_tab[...], stacked, preferred_element_type=jnp.float32)
        real, imag = wave[:N], wave[N:]
        density += weights[band] * (real * real + imag * imag)
    ordered = jnp.dot(
        density.astype(jnp.bfloat16), order[...], preferred_element_type=jnp.float32
    ).astype(jnp.bfloat16)
    own_rows = N // groups
    for owner in range(groups):
        sent[owner, plane] = ordered[owner * own_rows : (owner + 1) * own_rows]
    for step in range(1, groups):
        sum_copy(plane, step, group).start()

    @pl.when(plane == planes - 1)
    def _():
        def finish(which, carry):
            for step in range(1, groups):
                sum_copy(which, step, lax.rem(group + groups - step, groups)).wait()
            total = sent[group, which].astype(jnp.float32)
            for step in range(1, groups):
                total += landed[lax.rem(group + step, groups), which].astype(jnp.float32)
            out[which] = total
            return carry

        lax.fori_loop(0, total_planes, finish, 0)


def shards(coefficients, occupations, columns, counts, plane_slot):
    bands = coefficients.shape[0]
    here = columns.shape[0]
    ways = lax.axis_size("fft")
    groups = lax.axis_size("band")
    planes = plane_slot.shape[0] // ways
    live = LIVE_PER_DEVICE * ways
    coefficients = coefficients.reshape(bands, here, 2 * GB)
    plane_tab = stick_table(plane_slot)
    weights = occupations / (bands * groups)
    outgoing = jnp.einsum(
        "gjc,bsg->jcbs", plane_tab, coefficients, preferred_element_type=jnp.float32
    ).astype(jnp.bfloat16)
    outgoing = outgoing.reshape(ways, planes * 2 * bands, here)
    alive = jnp.arange(here, dtype=jnp.int32) < counts[0]
    meta = jnp.stack([columns // GB, columns % GB, alive.astype(jnp.int32)]).astype(jnp.bfloat16)
    meta = jnp.pad(meta, ((0, META - 3), (0, 0)))
    rows = N // groups
    chunk_planes = 6 if planes % 6 == 0 else planes
    chunks = planes // chunk_planes
    chunk_rows = chunk_planes * 2 * bands
    whole = pl.BlockSpec(memory_space=pltpu.VMEM)
    dma = pltpu.SemaphoreType.DMA
    return pl.pallas_call(
        functools.partial(grid_kernel, bands, live, chunk_planes, ways, groups),
        grid=(planes,),
        in_specs=[pl.BlockSpec(memory_space=pltpu.SMEM)] + [whole] * 5,
        out_specs=whole,
        out_shape=jax.ShapeDtypeStruct((planes, rows, N), jnp.float32),
        scratch_shapes=[
            pltpu.VMEM((chunks, ways, chunk_rows, here), jnp.bfloat16),
            pltpu.VMEM((ways, META, here), jnp.bfloat16),
            pltpu.VMEM((chunk_planes, 2 * bands, live), jnp.float32),
            pltpu.VMEM((live, 2 * LANES), jnp.bfloat16),
            pltpu.VMEM((2 * bands * GP, live), jnp.bfloat16),
            pltpu.VMEM((GP, live), jnp.float32),
            pltpu.VMEM((groups, planes, rows, N), jnp.bfloat16),
            pltpu.VMEM((groups, planes, rows, N), jnp.bfloat16),
            dma((ways - 1,)),
            dma((ways,)),
            dma((chunks, ways - 1)),
            dma((chunks, ways)),
            dma((planes, groups - 1)),
            dma((planes, groups)),
        ],
        compiler_params=pltpu.CompilerParams(
            vmem_limit_bytes=60 * 1024 * 1024, collective_id=0, has_side_effects=True
        ),
        name="grid",
    )(weights, outgoing, meta, row_table(), column_table(), order_table())


def solution(mesh):
    placed = (P("band", "fft"), P("band"), P("fft"), P("fft"), P())
    return jax.shard_map(
        shards, mesh=mesh, in_specs=placed, out_specs=P("fft", "band", None), check_vma=False
    )
```

```python
import functools
import math

import jax
import jax.numpy as jnp
import numpy as np
from jax import lax
from jax.experimental import pallas as pl
from jax.experimental.pallas import tpu as pltpu
from jax.sharding import PartitionSpec as P

N = 144
GB = 72
LIVE_PER_DEVICE = 64
GP = 80
YP = 256
META = 16
MESH = pl.DeviceIdType.MESH


def phase_pair(freq_count, positions, grid):
    freqs = jnp.arange(freq_count, dtype=jnp.int32) - freq_count // 2
    turns = jnp.mod(freqs[:, None] * positions[None, :], grid)
    angles = turns.astype(jnp.float32) * (2.0 * math.pi / grid)
    return (jnp.cos(angles), jnp.sin(angles))


def stick_table(plane_slot):
    valid_slot = (plane_slot >= 0).astype(jnp.float32)
    cosine, sine_part = phase_pair(GB, jnp.maximum(plane_slot, 0), N)
    cosine = cosine * valid_slot[None, :]
    sine_part = sine_part * valid_slot[None, :]
    upper = jnp.stack([cosine, sine_part], axis=-1)
    lower = jnp.stack([-sine_part, cosine], axis=-1)
    return jnp.concatenate([upper, lower], axis=0).astype(jnp.bfloat16)


def fixed_phases():
    freqs = np.arange(GB, dtype=np.int64) - GB // 2
    turns = np.mod(freqs[:, None] * np.arange(N)[None, :], N)
    angles = turns * (2.0 * math.pi / N)
    return np.cos(angles), np.sin(angles)


def row_table():
    cosine, sine_part = fixed_phases()
    table = np.zeros((GP, 4, YP))
    for place, part in enumerate((cosine, sine_part, -sine_part, cosine)):
        table[:GB, place, :N] = part
    return jnp.asarray(table.reshape(GP, 4 * YP).astype(jnp.bfloat16))


def column_table():
    cosine, sine_part = fixed_phases()
    table = np.zeros((2 * N, 2 * GP))
    table[:N, :GB] = cosine.T
    table[:N, GP : GP + GB] = -sine_part.T
    table[N:, :GB] = sine_part.T
    table[N:, GP : GP + GB] = cosine.T
    return jnp.asarray(table.astype(jnp.bfloat16))


def grid_kernel(
    bands, live, chunk_planes, ways, groups,
    weights, outgoing, meta_out, row_tab, col_tab,
    out,
    recv, meta_in, picks, sticks, table, masked, row_hot, sent, landed,
    meta_send, meta_recv, go_send, go_recv, sum_send, sum_recv,
):
    plane = pl.program_id(0)
    planes = pl.num_programs(0)
    total_planes = out.shape[0]
    chunks = total_planes // chunk_planes
    chunk_rows = chunk_planes * 2 * bands
    here = recv.shape[-1]
    me = lax.axis_index("fft")
    group = lax.axis_index("band")

    def meta_copy(step, source):
        peer = lax.rem(me + step, ways)
        return pltpu.make_async_remote_copy(
            src_ref=meta_out, dst_ref=meta_in.at[source],
            send_sem=meta_send.at[step - 1], recv_sem=meta_recv.at[source],
            device_id={"fft": peer}, device_id_type=MESH,
        )

    def stick_copy(chunk, step, source):
        peer = lax.rem(me + step, ways)
        return pltpu.make_async_remote_copy(
            src_ref=outgoing.at[peer, pl.ds(chunk * chunk_rows, chunk_rows)],
            dst_ref=recv.at[chunk, source],
            send_sem=go_send.at[chunk, step - 1], recv_sem=go_recv.at[chunk, source],
            device_id={"fft": peer}, device_id_type=MESH,
        )

    def sum_copy(which, step, source):
        peer = lax.rem(group + step, groups)
        return pltpu.make_async_remote_copy(
            src_ref=sent.at[peer, which], dst_ref=landed.at[source, which],
            send_sem=sum_send.at[which, step - 1], recv_sem=sum_recv.at[which, source],
            device_id={"band": peer}, device_id_type=MESH,
        )

    @pl.when(plane == 0)
    def _():
        barrier = pltpu.get_barrier_semaphore()
        for step in range(1, ways):
            pl.semaphore_signal(
                barrier, inc=1, device_id={"fft": lax.rem(me + step, ways)}, device_id_type=MESH
            )
        for step in range(1, groups):
            pl.semaphore_signal(
                barrier, inc=1, device_id={"band": lax.rem(group + step, groups)},
                device_id_type=MESH,
            )
        pl.semaphore_wait(barrier, ways + groups - 2)
        for step in range(1, ways):
            meta_copy(step, me).start()
        for chunk in range(chunks):
            for step in range(1, ways):
                stick_copy(chunk, step, me).start()
        meta_in[me] = meta_out[...]
        for chunk in range(chunks):
            recv[chunk, me] = outgoing[me, chunk * chunk_rows : (chunk + 1) * chunk_rows]
        for step in range(1, ways):
            meta_copy(step, lax.rem(me + ways - step, ways)).wait()

    @pl.when(lax.rem(plane, chunk_planes) == 0)
    def _():
        chunk = plane // chunk_planes
        for step in range(1, ways):
            stick_copy(chunk, step, lax.rem(me + ways - step, ways)).wait()
        turn = (((1,), (1,)), ((), ()))

        @pl.when(plane == 0)
        def _():
            offset = jnp.zeros((1, 1), jnp.float32)
            target = lax.broadcasted_iota(jnp.int32, (live, here), 0).astype(jnp.float32)
            place = lax.broadcasted_iota(jnp.int32, (1, here), 1).astype(jnp.float32)
            facts = jnp.zeros((META, live), jnp.float32)
            for source in range(ways):
                meta = meta_in[source]
                alive = meta.astype(jnp.float32)[2:3, :]
                spot = jnp.where(alive > 0.5, place + offset, -1.0)
                pick = jnp.where(target == spot, 1.0, 0.0).astype(jnp.bfloat16)
                picks[source] = pick
                facts += lax.dot_general(meta, pick, turn, preferred_element_type=jnp.float32)
                offset += jnp.sum(alive, axis=1, keepdims=True)
            freq = lax.broadcasted_iota(jnp.int32, (GP, live), 0).astype(jnp.float32)
            row_hot[...] = jnp.where(freq == facts[0:1, :], 1.0, 0.0)
            col_hot = jnp.where(freq == facts[1:2, :], 1.0, 0.0).astype(jnp.bfloat16)
            for part in range(2):
                table[part * live : (part + 1) * live, :] = lax.dot_general(
                    col_hot,
                    row_tab[:, 2 * YP * part : 2 * YP * (part + 1)],
                    (((0,), (0,)), ((), ())),
                    preferred_element_type=jnp.float32,
                ).astype(jnp.bfloat16)

        total = jnp.zeros((chunk_rows, live), jnp.float32)
        for source in range(ways):
            total += lax.dot_general(
                recv[chunk, source], picks[source], turn, preferred_element_type=jnp.float32
            )
        sticks[...] = total.reshape(sticks.shape)

    mine = sticks[lax.rem(plane, chunk_planes)]
    hot = row_hot[...]
    for part in range(2):
        for band in range(bands):
            row = mine[part * bands + band : part * bands + band + 1, :]
            masked[band * GP : (band + 1) * GP, part * live : (part + 1) * live] = (
                hot * row
            ).astype(jnp.bfloat16)
    half = jnp.dot(masked[...], table[...], preferred_element_type=jnp.float32)
    half = half.astype(jnp.bfloat16)
    density = jnp.zeros((N, YP), jnp.float32)
    for band in range(bands):
        piece = half[band * GP : (band + 1) * GP, :]
        stacked = jnp.concatenate([piece[:, :YP], piece[:, YP:]], axis=0)
        wave = jnp.dot(col_tab[...], stacked, preferred_element_type=jnp.float32)
        real, imag = wave[:N], wave[N:]
        density += weights[band] * (real * real + imag * imag)
    ordered = density[:, :N].astype(jnp.bfloat16)
    own_rows = N // groups
    for owner in range(groups):
        sent[owner, plane] = ordered[owner * own_rows : (owner + 1) * own_rows]
    for step in range(1, groups):
        sum_copy(plane, step, group).start()

    @pl.when(plane == planes - 1)
    def _():
        def finish(which, carry):
            for step in range(1, groups):
                sum_copy(which, step, lax.rem(group + groups - step, groups)).wait()
            total = sent[group, which].astype(jnp.float32)
            for step in range(1, groups):
                total += landed[lax.rem(group + step, groups), which].astype(jnp.float32)
            out[which] = total
            return carry

        lax.fori_loop(0, total_planes, finish, 0)


def shards(coefficients, occupations, columns, counts, plane_slot):
    bands = coefficients.shape[0]
    here = columns.shape[0]
    ways = lax.axis_size("fft")
    groups = lax.axis_size("band")
    planes = plane_slot.shape[0] // ways
    live = LIVE_PER_DEVICE * ways
    coefficients = coefficients.reshape(bands, here, 2 * GB)
    plane_tab = stick_table(plane_slot)
    weights = occupations / (bands * groups)
    outgoing = jnp.einsum(
        "gjc,bsg->jcbs", plane_tab, coefficients, preferred_element_type=jnp.float32
    ).astype(jnp.bfloat16)
    outgoing = outgoing.reshape(ways, planes * 2 * bands, here)
    alive = jnp.arange(here, dtype=jnp.int32) < counts[0]
    meta = jnp.stack([columns // GB, columns % GB, alive.astype(jnp.int32)]).astype(jnp.bfloat16)
    meta = jnp.pad(meta, ((0, META - 3), (0, 0)))
    rows = N // groups
    chunk_planes = 6 if planes % 6 == 0 else planes
    chunks = planes // chunk_planes
    chunk_rows = chunk_planes * 2 * bands
    whole = pl.BlockSpec(memory_space=pltpu.VMEM)
    dma = pltpu.SemaphoreType.DMA
    return pl.pallas_call(
        functools.partial(grid_kernel, bands, live, chunk_planes, ways, groups),
        grid=(planes,),
        in_specs=[pl.BlockSpec(memory_space=pltpu.SMEM)] + [whole] * 4,
        out_specs=whole,
        out_shape=jax.ShapeDtypeStruct((planes, rows, N), jnp.float32),
        scratch_shapes=[
            pltpu.VMEM((chunks, ways, chunk_rows, here), jnp.bfloat16),
            pltpu.VMEM((ways, META, here), jnp.bfloat16),
            pltpu.VMEM((ways, live, here), jnp.bfloat16),
            pltpu.VMEM((chunk_planes, 2 * bands, live), jnp.float32),
            pltpu.VMEM((2 * live, 2 * YP), jnp.bfloat16),
            pltpu.VMEM((bands * GP, 2 * live), jnp.bfloat16),
            pltpu.VMEM((GP, live), jnp.float32),
            pltpu.VMEM((groups, planes, rows, N), jnp.bfloat16),
            pltpu.VMEM((groups, planes, rows, N), jnp.bfloat16),
            dma((ways - 1,)),
            dma((ways,)),
            dma((chunks, ways - 1)),
            dma((chunks, ways)),
            dma((planes, groups - 1)),
            dma((planes, groups)),
        ],
        compiler_params=pltpu.CompilerParams(
            vmem_limit_bytes=60 * 1024 * 1024, collective_id=0, has_side_effects=True
        ),
        name="grid",
    )(weights, outgoing, meta, row_table(), column_table())


def solution(mesh):
    placed = (P("band", "fft"), P("band"), P("fft"), P("fft"), P())
    return jax.shard_map(
        shards, mesh=mesh, in_specs=placed, out_specs=P("fft", "band", None), check_vma=False
    )
```
